32 devices in a mesh: row: 4 (over y, x), col: 8 (over z, core).
Axes of the slice: x: 2, y: 2, z: 4, core: 2. Of those that a mesh axis runs over, the one named last changes fastest.
Arguments:
- density: bfloat16 [2048, 2048], P('row', 'col'), may hold values from -0.125 to 0.125
- density_mask: int32 [16, 16], P('row', 'col'), may hold values from 0 to 1, as said below
- response: bfloat16 [2, 2048, 2048], P(None, 'row', 'col'), may hold values from -6 to 6
- response_mask: int32 [2, 16, 16], P(None, 'row', 'col'), may hold values from 0 to 1, as said below
- filter_mask: int32 [16, 16], P('row', 'col'), may hold values from 0 to 1, as said below
Outputs:
- product: bfloat16 [2, 2048, 2048], P(None, 'row', 'col')
The draws below stay inside these ranges and needn't reach their ends.
Inputs may be any that keep to these rules, and one draw needn't show every extreme that they name: `density_mask`: diagonal blocks are always nonzero; blocks within cyclic block distance 2 of the diagonal are more often nonzero than blocks further out; whole block rows and whole block columns may be nonzero. `response_mask`: for each direction, diagonal blocks are always nonzero; blocks within cyclic block distance 2 of the diagonal are more often nonzero than blocks further out; whole block rows and whole block columns may be nonzero. `filter_mask`: diagonal blocks are always kept; blocks within cyclic block distance 2 * 2 of the diagonal are more often kept than blocks further out; whole block rows and whole block columns may be kept.
All inputs are finite; a program needn't handle non-finite values.
Results may differ from the reference program's by a relative error of at most 0.001.
Values may be sent and summed in bfloat16 or wider, within the bound.
A program may use at most 128 MiB of HBM per device.

```python
import jax
import jax.numpy as jnp

BLOCK = 128
NB_UNIT = 2
NB = 16
SLAB_ROWS = 4
BAND = 2
N = 2048


def banded_pattern(key, keep_near, keep_far, reach):
    first = jnp.arange(NB, dtype=jnp.int32)[:, None]
    second = jnp.arange(NB, dtype=jnp.int32)[None, :]
    spacing = jnp.abs(first - second)
    distance = jnp.minimum(spacing, NB - spacing)
    rolled = jax.random.randint(jax.random.fold_in(key, 1), (NB, NB), 0, 100, dtype=jnp.int32)
    kept = jnp.where(distance <= reach, rolled < keep_near, rolled < keep_far)
    kept = jnp.logical_or(kept, distance == 0)
    row_group = jax.random.randint(jax.random.fold_in(key, 2), (), 0, NB // SLAB_ROWS, dtype=jnp.int32)
    col_group = jax.random.randint(jax.random.fold_in(key, 3), (), 0, NB // NB_UNIT, dtype=jnp.int32)
    full_rows = first // SLAB_ROWS == row_group
    full_cols = second // NB_UNIT == col_group
    kept = jnp.logical_or(kept, jnp.logical_or(full_rows, full_cols))
    return kept.astype(jnp.int32)


def draw_density_mask(key, part):
    return banded_pattern(jax.random.fold_in(key, 11), 80, 8, BAND)


def draw_response_mask(key, part):
    first = banded_pattern(jax.random.fold_in(key, 21), 80, 8, BAND)
    second = banded_pattern(jax.random.fold_in(key, 22), 80, 8, BAND)
    return jnp.stack([first, second])


def draw_filter_mask(key, part):
    return banded_pattern(jax.random.fold_in(key, 31), 90, 25, 2 * BAND)


def block_levels(key, shape, shards, low, high):
    def one(position, blocks):
        draws = jax.random.uniform(jax.random.fold_in(jax.random.fold_in(key, 6), position), (blocks,), jnp.float32, low / len(shards), high / len(shards))
        return jnp.repeat(jnp.exp(draws), shape[position] // blocks).reshape((-1,) + (1,) * (len(shape) - position - 1))

    factor_of = one(*shards[0])
    for cut in shards[1:]:
        factor_of = factor_of * one(*cut)
    return factor_of


def noise(rng, shape, spread, most, pieces=(), kind=jnp.bfloat16):
    drawn = jax.random.normal(rng, shape, jnp.float32) * spread
    if len(pieces) > 0:
        drawn = block_levels(rng, shape, pieces, -0.22, 0.18) * drawn
    return jnp.clip(drawn, min=-most, max=most).astype(kind)


def setup_inputs(seed: int = 0) -> dict:
    key_of = jax.random.split(jax.random.key(seed), 6)
    density = noise(key_of[0], (N, N), N ** -0.5, 0.125, ((0, 4), (1, 8)))
    density_mask = draw_density_mask(jax.random.fold_in(key_of[5], 71), 0)
    response = noise(key_of[2], (2, N, N), 1.0, 6.0, ((1, 4), (2, 8)))
    response_mask = draw_response_mask(jax.random.fold_in(key_of[5], 71), 0)
    filter_mask = draw_filter_mask(jax.random.fold_in(key_of[5], 71), 0)
    return dict(density=density, density_mask=density_mask, response=response, response_mask=response_mask, filter_mask=filter_mask)


def expand_blocks(values, mask, blocksize):
    lead = values.shape[:-2]
    height = values.shape[-2] // blocksize
    width = values.shape[-1] // blocksize
    shaped = values.reshape(lead + (height, blocksize, width, blocksize))
    scaled = shaped * mask.astype(values.dtype)[..., :, None, :, None]
    return scaled.reshape(values.shape)


def reference(density, density_mask, response, response_mask, filter_mask):
    masked_density = expand_blocks(density, density_mask, BLOCK)
    masked_response = expand_blocks(response, response_mask, BLOCK)
    first = jnp.dot(masked_density, masked_response[0], preferred_element_type=jnp.float32)
    second = jnp.dot(masked_density, masked_response[1], preferred_element_type=jnp.float32)
    stacked = jnp.stack([first, second])
    return expand_blocks(stacked, filter_mask, BLOCK).astype(jnp.bfloat16)
```

```python
import functools

import jax
import jax.numpy as jnp
from jax import lax
from jax.experimental import pallas as pl
from jax.experimental.pallas import tpu as pltpu
from jax.sharding import PartitionSpec as P

CORES = 2
HALVES = 2


def kernel(
    ring, cols, density, density_mask, response, response_mask, filter_mask,
    out, a_full, b_full, acc, load_sem,
    a_send, a_recv, b_send, b_recv, d_send, d_recv,
):
    chips = cols // CORES
    dirs, depth, width = response.shape
    rows, kblock = density.shape
    piece = rows // HALVES
    per = depth // kblock
    nb = dirs * per
    far = ring // 2
    a_items = HALVES * (chips - 1)
    b_items = nb * (far - 1) + nb // 2
    blk_r = rows // density_mask.shape[0]
    blk_k = kblock // density_mask.shape[1]

    row = lax.axis_index("row")
    col = lax.axis_index("col")
    chip, core = col // CORES, col % CORES
    partner = chip * CORES + (CORES - 1 - core)

    def row_of(pos):
        pos = lax.rem(pos + 2 * ring, ring)
        return jnp.where(pos < far, 2 * pos, 2 * (ring - 1 - pos) + 1)

    def pos_of(r):
        return jnp.where(r % 2 == 0, r // 2, ring - 1 - r // 2)

    pos = pos_of(row)
    next_row, prev_row = row_of(pos + 1), row_of(pos - 1)
    has_up, has_down = chip < chips - 1, chip > 0

    barrier = pltpu.get_barrier_semaphore()
    pl.semaphore_signal(barrier, inc=1, device_id={"row": next_row})
    pl.semaphore_signal(barrier, inc=1, device_id={"row": prev_row})
    pl.semaphore_signal(barrier, inc=1, device_id={"col": partner})

    @pl.when(has_up)
    def _():
        pl.semaphore_signal(barrier, inc=1, device_id={"col": col + CORES})

    @pl.when(has_down)
    def _():
        pl.semaphore_signal(barrier, inc=1, device_id={"col": col - CORES})

    load_a = pltpu.make_async_copy(density, a_full.at[col], load_sem.at[0])
    load_b = pltpu.make_async_copy(response, b_full.at[row], load_sem.at[1])
    load_a.start()
    load_b.start()
    acc[...] = jnp.zeros_like(acc)
    load_a.wait()
    for i in range(rows // blk_r):
        for k in range(kblock // blk_k):
            part = (col, pl.ds(i * blk_r, blk_r), pl.ds(k * blk_k, blk_k))
            factor = jnp.full((blk_r, blk_k), density_mask[i, k].astype(jnp.float32)).astype(jnp.bfloat16)
            a_full[part] = a_full[part] * factor
    load_b.wait()
    for d in range(dirs):
        for i in range(depth // blk_k):
            for k in range(width // blk_k):
                part = (row, d, pl.ds(i * blk_k, blk_k), pl.ds(k * blk_k, blk_k))
                factor = jnp.full((blk_k, blk_k), response_mask[d, i, k].astype(jnp.float32)).astype(jnp.bfloat16)
                b_full[part] = b_full[part] * factor
    pl.semaphore_wait(barrier, 3 + has_up.astype(jnp.int32) + has_down.astype(jnp.int32))

    def a_copy(way, item):
        step, half = item // HALVES, item % HALVES
        sign = 1 - 2 * way
        origin = (chip - sign * step) * CORES + core
        ref = a_full.at[origin, pl.ds(pl.multiple_of(half * piece, piece), piece)]
        return pltpu.make_async_remote_copy(
            ref, ref, a_send.at[way, item], a_recv.at[way, item],
            device_id={"col": col + sign * CORES},
        )

    def a_arrival(way, item):
        step, half = item // HALVES, item % HALVES
        sign = 1 - 2 * way
        origin = (chip - sign * (step + 1)) * CORES + core
        ref = a_full.at[origin, pl.ds(pl.multiple_of(half * piece, piece), piece)]
        return pltpu.make_async_remote_copy(
            ref, ref, a_send.at[way, item], a_recv.at[way, item],
            device_id={"col": col + sign * CORES},
        )

    def d_copy(origin_chip, half, whose):
        ref = a_full.at[origin_chip * CORES + whose, pl.ds(pl.multiple_of(half * piece, piece), piece)]
        return pltpu.make_async_remote_copy(
            ref, ref, d_send.at[origin_chip, half], d_recv.at[origin_chip, half],
            device_id={"col": partner},
        )

    def b_ref(way, item, origin_pos):
        j = item % nb
        d, s = j // per, j % per
        if way == 1:
            d = dirs - 1 - d
        return b_full.at[row_of(origin_pos), d, pl.ds(pl.multiple_of(s * kblock, kblock), kblock)]

    def b_copy(way, item):
        sign = 1 - 2 * way
        ref = b_ref(way, item, pos - sign * (item // nb))
        return pltpu.make_async_remote_copy(
            ref, ref, b_send.at[way, item], b_recv.at[way, item],
            device_id={"row": next_row if way == 0 else prev_row},
        )

    def b_arrival(way, item):
        sign = 1 - 2 * way
        ref = b_ref(way, item, pos - sign * (item // nb + 1))
        return pltpu.make_async_remote_copy(
            ref, ref, b_send.at[way, item], b_recv.at[way, item],
            device_id={"row": next_row if way == 0 else prev_row},
        )

    own_b = min(nb, b_items)
    for item in range(max(own_b, HALVES)):
        if item < HALVES and chips > 1:
            pl.when(has_up)(lambda item=item: a_copy(0, item).start())
            pl.when(has_down)(lambda item=item: a_copy(1, item).start())
        if item < own_b:
            b_copy(0, item).start()
            b_copy(1, item).start()
    for half in range(HALVES):
        d_copy(chip, half, core).start()

    def ready(origin_chip, d):
        t_a = HALVES * jnp.abs(origin_chip - chip)
        source = (origin_chip * CORES) // per
        gap = lax.rem(pos - pos_of(source) + ring, ring)
        from_prev = (gap - 1) * nb + (d + 1) * per
        from_next = (ring - gap - 1) * nb + (dirs - d) * per
        up = jnp.logical_or(gap < far, jnp.logical_and(gap == far, d < dirs // 2))
        t_b = jnp.where(gap == 0, 0, jnp.where(up, from_prev, from_next))
        return jnp.maximum(t_a, t_b)

    def compute(tick):
        def unit(index, carry):
            o, d = index // dirs, index % dirs

            @pl.when(ready(o, d) == tick)
            def _():
                source = (o * CORES) // per
                s = (o * CORES) % per
                total = acc[d]
                for c in range(CORES):
                    total += jnp.dot(
                        a_full[o * CORES + c],
                        b_full[source, d, pl.ds(pl.multiple_of((s + c) * kblock, kblock), kblock)],
                        preferred_element_type=jnp.float32,
                    )
                acc[d] = total
            return carry

        lax.fori_loop(0, chips * dirs, unit, 0)

    ticks = max(a_items, b_items)

    def step(tick, carry):
        item = tick - 1

        @pl.when(tick > 0)
        def _():
            for way in range(2):
                sign = 1 - 2 * way
                origin = chip - sign * (item // HALVES + 1)
                here = jnp.logical_and(item < a_items, jnp.logical_and(origin >= 0, origin < chips))

                @pl.when(here)
                def _():
                    a_arrival(way, item).wait_recv()

                    @pl.when(has_up if way == 0 else has_down)
                    def _():
                        a_copy(way, item + HALVES).start()

                    d_copy(origin, item % HALVES, core).start()

            @pl.when(item < b_items)
            def _():
                for way in range(2):
                    b_arrival(way, item).wait_recv()

                    @pl.when(item + nb < b_items)
                    def _():
                        b_copy(way, item + nb).start()

            for way in range(2):
                sign = 1 - 2 * way
                origin = chip - sign * (item // HALVES + 1)
                here = jnp.logical_and(item < a_items, jnp.logical_and(origin >= 0, origin < chips))

                @pl.when(here)
                def _():
                    d_copy(origin, item % HALVES, CORES - 1 - core).wait_recv()

        @pl.when(tick == 0)
        def _():
            for half in range(HALVES):
                d_copy(chip, half, CORES - 1 - core).wait_recv()

        compute(tick)
        return carry

    lax.fori_loop(0, ticks + 1, step, 0)

    blk_m, blk_n = rows // filter_mask.shape[0], width // filter_mask.shape[1]
    for d in range(dirs):
        for i in range(rows // blk_m):
            for k in range(width // blk_n):
                part = (d, pl.ds(i * blk_m, blk_m), pl.ds(k * blk_n, blk_n))
                out[part] = (acc[part] * filter_mask[i, k].astype(jnp.float32)).astype(jnp.bfloat16)

    def drain_a(item, carry):
        for way in range(2):
            sign = 1 - 2 * way
            origin = chip - sign * (item // HALVES)
            sent = jnp.logical_and(has_up if way == 0 else has_down, jnp.logical_and(origin >= 0, origin < chips))
            pl.when(sent)(lambda way=way: a_copy(way, item).wait_send())
        return carry

    def drain_b(item, carry):
        for way in range(2):
            b_copy(way, item).wait_send()
        return carry

    def drain_d(index, carry):
        d_copy(index // HALVES, index % HALVES, core).wait_send()
        return carry

    lax.fori_loop(0, a_items, drain_a, 0)
    lax.fori_loop(0, b_items, drain_b, 0)
    lax.fori_loop(0, chips * HALVES, drain_d, 0)


def solution(mesh):
    ring, cols = mesh.shape["row"], mesh.shape["col"]

    def body(density, density_mask, response, response_mask, filter_mask):
        dirs, depth, width = response.shape
        rows, kblock = density.shape
        chips = cols // CORES
        nb = dirs * (depth // kblock)
        a_items = HALVES * (chips - 1)
        b_items = nb * (ring // 2 - 1) + nb // 2
        dma = pltpu.SemaphoreType.DMA
        hbm = pl.BlockSpec(memory_space=pl.ANY)
        smem = pl.BlockSpec(memory_space=pltpu.SMEM)
        return pl.pallas_call(
            functools.partial(kernel, ring, cols),
            out_shape=jax.ShapeDtypeStruct((dirs, rows, width), jnp.bfloat16),
            in_specs=[hbm, smem, hbm, smem, smem],
            out_specs=pl.BlockSpec(memory_space=pltpu.VMEM),
            scratch_shapes=[
                pltpu.VMEM((cols, rows, kblock), jnp.bfloat16),
                pltpu.VMEM((ring, dirs, depth, width), jnp.bfloat16),
                pltpu.VMEM((dirs, rows, width), jnp.float32),
                dma((2,)),
                dma((2, a_items)),
                dma((2, a_items)),
                dma((2, b_items)),
                dma((2, b_items)),
                dma((chips, HALVES)),
                dma((chips, HALVES)),
            ],
            compiler_params=pltpu.CompilerParams(collective_id=0, has_side_effects=True),
        )(density, density_mask, response, response_mask, filter_mask)

    return jax.shard_map(
        body,
        mesh=mesh,
        in_specs=(P("row", "col"), P("row", "col"), P(None, "row", "col"), P(None, "row", "col"), P("row", "col")),
        out_specs=P(None, "row", "col"),
        check_vma=False,
    )
```

```python
import functools

import jax
import jax.numpy as jnp
from jax import lax
from jax.experimental import pallas as pl
from jax.experimental.pallas import tpu as pltpu
from jax.sharding import PartitionSpec as P

CORES = 2
HALVES = 2


def kernel(
    ring, cols, density, density_mask, response, response_mask, filter_mask,
    out, a_full, b_full, acc, load_sem,
    a_send, a_recv, b_send, b_recv, d_send, d_recv,
):
    chips = cols // CORES
    dirs, depth, width = response.shape
    rows, kblock = density.shape
    piece = rows // HALVES
    per = depth // kblock
    nb = dirs * per
    far = ring // 2
    a_items = HALVES * (chips - 1)
    b_items = nb * (far - 1) + nb // 2
    blk_r = rows // density_mask.shape[1]
    blk_k = kblock // density_mask.shape[0]

    row = lax.axis_index("row")
    col = lax.axis_index("col")
    chip, core = col // CORES, col % CORES
    partner = chip * CORES + (CORES - 1 - core)

    def row_of(pos):
        pos = lax.rem(pos + 2 * ring, ring)
        return jnp.where(pos < far, 2 * pos, 2 * (ring - 1 - pos) + 1)

    def pos_of(r):
        return jnp.where(r % 2 == 0, r // 2, ring - 1 - r // 2)

    pos = pos_of(row)
    next_row, prev_row = row_of(pos + 1), row_of(pos - 1)
    has_up, has_down = chip < chips - 1, chip > 0

    barrier = pltpu.get_barrier_semaphore()
    pl.semaphore_signal(barrier, inc=1, device_id={"row": next_row})
    pl.semaphore_signal(barrier, inc=1, device_id={"row": prev_row})
    pl.semaphore_signal(barrier, inc=1, device_id={"col": partner})

    @pl.when(has_up)
    def _():
        pl.semaphore_signal(barrier, inc=1, device_id={"col": col + CORES})

    @pl.when(has_down)
    def _():
        pl.semaphore_signal(barrier, inc=1, device_id={"col": col - CORES})

    load_a = pltpu.make_async_copy(density, a_full.at[col], load_sem.at[0])
    load_b = pltpu.make_async_copy(response, b_full.at[row], load_sem.at[1])
    load_a.start()
    load_b.start()
    acc[...] = jnp.zeros_like(acc)
    load_a.wait()
    for i in range(rows // blk_r):
        for k in range(kblock // blk_k):
            part = (col, pl.ds(i * blk_r, blk_r), pl.ds(k * blk_k, blk_k))
            factor = jnp.full((blk_r, blk_k), density_mask[k, i].astype(jnp.float32)).astype(jnp.bfloat16)
            a_full[part] = a_full[part] * factor
    load_b.wait()
    for d in range(dirs):
        for i in range(depth // blk_k):
            for k in range(width // blk_k):
                part = (row, d, pl.ds(i * blk_k, blk_k), pl.ds(k * blk_k, blk_k))
                factor = jnp.full((blk_k, blk_k), response_mask[d, k, i].astype(jnp.float32)).astype(jnp.bfloat16)
                b_full[part] = b_full[part] * factor
    pl.semaphore_wait(barrier, 3 + has_up.astype(jnp.int32) + has_down.astype(jnp.int32))

    def a_copy(way, item):
        step, half = item // HALVES, item % HALVES
        sign = 1 - 2 * way
        origin = (chip - sign * step) * CORES + core
        ref = a_full.at[origin, pl.ds(pl.multiple_of(half * piece, piece), piece)]
        return pltpu.make_async_remote_copy(
            ref, ref, a_send.at[way, item], a_recv.at[way, item],
            device_id={"col": col + sign * CORES},
        )

    def a_arrival(way, item):
        step, half = item // HALVES, item % HALVES
        sign = 1 - 2 * way
        origin = (chip - sign * (step + 1)) * CORES + core
        ref = a_full.at[origin, pl.ds(pl.multiple_of(half * piece, piece), piece)]
        return pltpu.make_async_remote_copy(
            ref, ref, a_send.at[way, item], a_recv.at[way, item],
            device_id={"col": col + sign * CORES},
        )

    def d_copy(origin_chip, half, whose):
        ref = a_full.at[origin_chip * CORES + whose, pl.ds(pl.multiple_of(half * piece, piece), piece)]
        return pltpu.make_async_remote_copy(
            ref, ref, d_send.at[origin_chip, half], d_recv.at[origin_chip, half],
            device_id={"col": partner},
        )

    def b_ref(way, item, origin_pos):
        j = item % nb
        d, s = j // per, j % per
        if way == 1:
            d = dirs - 1 - d
        return b_full.at[row_of(origin_pos), d, pl.ds(pl.multiple_of(s * kblock, kblock), kblock)]

    def b_copy(way, item):
        sign = 1 - 2 * way
        ref = b_ref(way, item, pos - sign * (item // nb))
        return pltpu.make_async_remote_copy(
            ref, ref, b_send.at[way, item], b_recv.at[way, item],
            device_id={"row": next_row if way == 0 else prev_row},
        )

    def b_arrival(way, item):
        sign = 1 - 2 * way
        ref = b_ref(way, item, pos - sign * (item // nb + 1))
        return pltpu.make_async_remote_copy(
            ref, ref, b_send.at[way, item], b_recv.at[way, item],
            device_id={"row": next_row if way == 0 else prev_row},
        )

    own_b = min(nb, b_items)
    for item in range(max(own_b, HALVES)):
        if item < HALVES and chips > 1:
            pl.when(has_up)(lambda item=item: a_copy(0, item).start())
            pl.when(has_down)(lambda item=item: a_copy(1, item).start())
        if item < own_b:
            b_copy(0, item).start()
            b_copy(1, item).start()
    for half in range(HALVES):
        d_copy(chip, half, core).start()

    def ready(origin_chip, d):
        t_a = HALVES * jnp.abs(origin_chip - chip)
        source = (origin_chip * CORES) // per
        gap = lax.rem(pos - pos_of(source) + ring, ring)
        from_prev = (gap - 1) * nb + (d + 1) * per
        from_next = (ring - gap - 1) * nb + (dirs - d) * per
        up = jnp.logical_or(gap < far, jnp.logical_and(gap == far, d < dirs // 2))
        t_b = jnp.where(gap == 0, 0, jnp.where(up, from_prev, from_next))
        return jnp.maximum(t_a, t_b)

    def compute(tick):
        def unit(index, carry):
            o, d = index // dirs, index % dirs

            @pl.when(ready(o, d) == tick)
            def _():
                source = (o * CORES) // per
                s = (o * CORES) % per
                total = acc[d]
                for c in range(CORES):
                    total += jnp.dot(
                        a_full[o * CORES + c],
                        b_full[source, d, pl.ds(pl.multiple_of((s + c) * kblock, kblock), kblock)],
                        preferred_element_type=jnp.float32,
                    )
                acc[d] = total
            return carry

        lax.fori_loop(0, chips * dirs, unit, 0)

    ticks = max(a_items, b_items)

    def step(tick, carry):
        item = tick - 1

        @pl.when(tick > 0)
        def _():
            for way in range(2):
                sign = 1 - 2 * way
                origin = chip - sign * (item // HALVES + 1)
                here = jnp.logical_and(item < a_items, jnp.logical_and(origin >= 0, origin < chips))

                @pl.when(here)
                def _():
                    a_arrival(way, item).wait_recv()

                    @pl.when(has_up if way == 0 else has_down)
                    def _():
                        a_copy(way, item + HALVES).start()

                    d_copy(origin, item % HALVES, core).start()

            @pl.when(item < b_items)
            def _():
                for way in range(2):
                    b_arrival(way, item).wait_recv()

                    @pl.when(item + nb < b_items)
                    def _():
                        b_copy(way, item + nb).start()

            for way in range(2):
                sign = 1 - 2 * way
                origin = chip - sign * (item // HALVES + 1)
                here = jnp.logical_and(item < a_items, jnp.logical_and(origin >= 0, origin < chips))

                @pl.when(here)
                def _():
                    d_copy(origin, item % HALVES, CORES - 1 - core).wait_recv()

        @pl.when(tick == 0)
        def _():
            for half in range(HALVES):
                d_copy(chip, half, CORES - 1 - core).wait_recv()

        compute(tick)
        return carry

    lax.fori_loop(0, ticks + 1, step, 0)

    blk_m, blk_n = rows // filter_mask.shape[1], width // filter_mask.shape[0]
    for d in range(dirs):
        for i in range(rows // blk_m):
            for k in range(width // blk_n):
                part = (d, pl.ds(i * blk_m, blk_m), pl.ds(k * blk_n, blk_n))
                out[part] = (acc[part] * filter_mask[k, i].astype(jnp.float32)).astype(jnp.bfloat16)

    def drain_a(item, carry):
        for way in range(2):
            sign = 1 - 2 * way
            origin = chip - sign * (item // HALVES)
            sent = jnp.logical_and(has_up if way == 0 else has_down, jnp.logical_and(origin >= 0, origin < chips))
            pl.when(sent)(lambda way=way: a_copy(way, item).wait_send())
        return carry

    def drain_b(item, carry):
        for way in range(2):
            b_copy(way, item).wait_send()
        return carry

    def drain_d(index, carry):
        d_copy(index // HALVES, index % HALVES, core).wait_send()
        return carry

    lax.fori_loop(0, a_items, drain_a, 0)
    lax.fori_loop(0, b_items, drain_b, 0)
    lax.fori_loop(0, chips * HALVES, drain_d, 0)


def solution(mesh):
    ring, cols = mesh.shape["row"], mesh.shape["col"]

    def body(density, density_mask, response, response_mask, filter_mask):
        dirs, depth, width = response.shape
        rows, kblock = density.shape
        chips = cols // CORES
        nb = dirs * (depth // kblock)
        a_items = HALVES * (chips - 1)
        b_items = nb * (ring // 2 - 1) + nb // 2
        dma = pltpu.SemaphoreType.DMA
        hbm = pl.BlockSpec(memory_space=pl.ANY)
        smem = pl.BlockSpec(memory_space=pltpu.SMEM)
        return pl.pallas_call(
            functools.partial(kernel, ring, cols),
            out_shape=pltpu.VMEM((dirs, rows, width), jnp.bfloat16),
            in_specs=[hbm, smem, hbm, smem, smem],
            out_specs=pl.BlockSpec(memory_space=pltpu.VMEM),
            scratch_shapes=[
                pltpu.VMEM((cols, rows, kblock), jnp.bfloat16),
                pltpu.VMEM((ring, dirs, depth, width), jnp.bfloat16),
                pltpu.VMEM((dirs, rows, width), jnp.float32),
                dma((2,)),
                dma((2, a_items)),
                dma((2, a_items)),
                dma((2, b_items)),
                dma((2, b_items)),
                dma((chips, HALVES)),
                dma((chips, HALVES)),
            ],
            compiler_params=pltpu.CompilerParams(collective_id=0, has_side_effects=True),
        )(density, density_mask.T, response, jnp.swapaxes(response_mask, 1, 2), filter_mask.T)

    return jax.shard_map(
        body,
        mesh=mesh,
        in_specs=(P("row", "col"), P("row", "col"), P(None, "row", "col"), P(None, "row", "col"), P("row", "col")),
        out_specs=P(None, "row", "col"),
        check_vma=False,
    )
```

```python
import functools

import jax
import jax.numpy as jnp
from jax import lax
from jax.experimental import pallas as pl
from jax.experimental.pallas import tpu as pltpu
from jax.sharding import PartitionSpec as P

CORES = 2
PIECES = 4
SPLIT = 2


def kernel(
    ring, cols, density, density_mask_in, response, response_mask_in, filter_mask_in,
    out, density_mask, response_mask, filter_mask, a_full, b_full, acc, load_sem,
    a_send, a_recv, b_send, b_recv, d_send, d_recv,
):
    chips = cols // CORES
    dirs, depth, width = response.shape
    rows, kblock = density.shape
    piece = rows // PIECES
    per = depth // kblock
    thin = kblock // SPLIT
    nb = dirs * per * SPLIT
    far = ring // 2
    a_items = PIECES * (chips - 1)
    b_items = nb * (far - 1) + nb // 2
    blk_r = rows // density_mask.shape[1]
    blk_k = kblock // density_mask.shape[0]

    row = lax.axis_index("row")
    col = lax.axis_index("col")
    chip, core = col // CORES, col % CORES
    partner = chip * CORES + (CORES - 1 - core)

    def row_of(pos):
        pos = lax.rem(pos + 2 * ring, ring)
        return jnp.where(pos < far, 2 * pos, 2 * (ring - 1 - pos) + 1)

    def pos_of(r):
        return jnp.where(r % 2 == 0, r // 2, ring - 1 - r // 2)

    pos = pos_of(row)
    next_row, prev_row = row_of(pos + 1), row_of(pos - 1)
    has_up, has_down = chip < chips - 1, chip > 0

    barrier = pltpu.get_barrier_semaphore()
    pl.semaphore_signal(barrier, inc=1, device_id={"row": next_row})
    pl.semaphore_signal(barrier, inc=1, device_id={"row": prev_row})
    pl.semaphore_signal(barrier, inc=1, device_id={"col": partner})

    @pl.when(has_up)
    def _():
        pl.semaphore_signal(barrier, inc=1, device_id={"col": col + CORES})

    @pl.when(has_down)
    def _():
        pl.semaphore_signal(barrier, inc=1, device_id={"col": col - CORES})

    load_a = pltpu.make_async_copy(density, a_full.at[col], load_sem.at[0])
    load_b = pltpu.make_async_copy(response, b_full.at[row], load_sem.at[1])
    load_masks = [
        pltpu.make_async_copy(source, target, load_sem.at[2 + i])
        for i, (source, target) in enumerate((
            (density_mask_in, density_mask), (response_mask_in, response_mask), (filter_mask_in, filter_mask)))
    ]
    load_a.start()
    load_masks[0].start()
    load_masks[1].start()
    load_b.start()
    load_masks[2].start()
    acc[...] = jnp.zeros_like(acc)
    load_a.wait()
    load_masks[0].wait()
    for i in range(rows // blk_r):
        for k in range(kblock // blk_k):
            part = (col, pl.ds(i * blk_r, blk_r), pl.ds(k * blk_k, blk_k))
            factor = jnp.full((blk_r, blk_k), density_mask[k, i].astype(jnp.float32)).astype(jnp.bfloat16)
            a_full[part] = a_full[part] * factor
    load_b.wait()
    load_masks[1].wait()
    load_masks[2].wait()
    for d in range(dirs):
        for i in range(depth // blk_k):
            for k in range(width // blk_k):
                part = (row, d, pl.ds(i * blk_k, blk_k), pl.ds(k * blk_k, blk_k))
                factor = jnp.full((blk_k, blk_k), response_mask[d, k, i].astype(jnp.float32)).astype(jnp.bfloat16)
                b_full[part] = b_full[part] * factor
    pl.semaphore_wait(barrier, 3 + has_up.astype(jnp.int32) + has_down.astype(jnp.int32))

    def a_copy(way, item):
        step, half = item // PIECES, item % PIECES
        sign = 1 - 2 * way
        origin = (chip - sign * step) * CORES + core
        ref = a_full.at[origin, pl.ds(pl.multiple_of(half * piece, piece), piece)]
        return pltpu.make_async_remote_copy(
            ref, ref, a_send.at[way, item], a_recv.at[way, item],
            device_id={"col": col + sign * CORES},
        )

    def a_arrival(way, item):
        step, half = item // PIECES, item % PIECES
        sign = 1 - 2 * way
        origin = (chip - sign * (step + 1)) * CORES + core
        ref = a_full.at[origin, pl.ds(pl.multiple_of(half * piece, piece), piece)]
        return pltpu.make_async_remote_copy(
            ref, ref, a_send.at[way, item], a_recv.at[way, item],
            device_id={"col": col + sign * CORES},
        )

    def d_copy(origin_chip, half, whose):
        ref = a_full.at[origin_chip * CORES + whose, pl.ds(pl.multiple_of(half * piece, piece), piece)]
        return pltpu.make_async_remote_copy(
            ref, ref, d_send.at[origin_chip, half], d_recv.at[origin_chip, half],
            device_id={"col": partner},
        )

    def b_ref(way, item, origin_pos):
        j = item % nb
        d, s = j // (per * SPLIT), j % (per * SPLIT)
        if way == 1:
            d = dirs - 1 - d
        return b_full.at[row_of(origin_pos), d, pl.ds(pl.multiple_of(s * thin, thin), thin)]

    def b_copy(way, item):
        sign = 1 - 2 * way
        ref = b_ref(way, item, pos - sign * (item // nb))
        return pltpu.make_async_remote_copy(
            ref, ref, b_send.at[way, item], b_recv.at[way, item],
            device_id={"row": next_row if way == 0 else prev_row},
        )

    def b_arrival(way, item):
        sign = 1 - 2 * way
        ref = b_ref(way, item, pos - sign * (item // nb + 1))
        return pltpu.make_async_remote_copy(
            ref, ref, b_send.at[way, item], b_recv.at[way, item],
            device_id={"row": next_row if way == 0 else prev_row},
        )

    own_b = min(nb, b_items)
    for item in range(max(own_b, PIECES)):
        if item < PIECES and chips > 1:
            pl.when(has_up)(lambda item=item: a_copy(0, item).start())
            pl.when(has_down)(lambda item=item: a_copy(1, item).start())
        if item < own_b:
            b_copy(0, item).start()
            b_copy(1, item).start()
    for half in range(PIECES):
        d_copy(chip, half, core).start()

    def ready(origin_chip, c, d, source, s):
        late = jnp.where(c == core, 0, 1)
        t_a = PIECES * jnp.abs(origin_chip - chip) + late
        gap = lax.rem(pos - pos_of(source) + ring, ring)
        from_prev = (gap - 1) * nb + (d * per + s + 1) * SPLIT
        from_next = (ring - gap - 1) * nb + ((dirs - 1 - d) * per + s + 1) * SPLIT
        up = jnp.logical_or(gap < far, jnp.logical_and(gap == far, d < dirs // 2))
        t_b = jnp.where(gap == 0, 0, jnp.where(up, from_prev, from_next))
        return jnp.maximum(t_a, t_b)

    def compute(tick):
        def unit(index, carry):
            d, k = index % dirs, index // dirs
            o, c = k // CORES, k % CORES
            source, s = k // per, k % per

            @pl.when(ready(o, c, d, source, s) == tick)
            def _():
                acc[d] += jnp.dot(
                    a_full[k],
                    b_full[source, d, pl.ds(pl.multiple_of(s * kblock, kblock), kblock)],
                    preferred_element_type=jnp.float32,
                )
            return carry

        lax.fori_loop(0, cols * dirs, unit, 0)

    ticks = max(a_items + 1, b_items)

    def arrives(way, item):
        origin = chip - (1 - 2 * way) * (item // PIECES + 1)
        inside = jnp.logical_and(origin >= 0, origin < chips)
        return origin, jnp.logical_and(jnp.logical_and(item >= 0, item < a_items), inside)

    def step(tick, carry):
        item = tick - 1
        for way in range(2):
            origin, here = arrives(way, item)

            @pl.when(here)
            def _():
                a_arrival(way, item).wait_recv()

                @pl.when(has_up if way == 0 else has_down)
                def _():
                    a_copy(way, item + PIECES).start()

                d_copy(origin, item % PIECES, core).start()

        @pl.when(jnp.logical_and(item >= 0, item < b_items))
        def _():
            for way in range(2):
                b_arrival(way, item).wait_recv()

                @pl.when(item + nb < b_items)
                def _():
                    b_copy(way, item + nb).start()

        for way in range(2):
            origin, here = arrives(way, item - 1)

            @pl.when(here)
            def _():
                d_copy(origin, (item - 1) % PIECES, CORES - 1 - core).wait_recv()

        @pl.when(tick == 1)
        def _():
            for part in range(PIECES):
                d_copy(chip, part, CORES - 1 - core).wait_recv()

        compute(tick)
        return carry

    lax.fori_loop(0, ticks + 1, step, 0)

    blk_m, blk_n = rows // filter_mask.shape[1], width // filter_mask.shape[0]
    for d in range(dirs):
        for i in range(rows // blk_m):
            for k in range(width // blk_n):
                part = (d, pl.ds(i * blk_m, blk_m), pl.ds(k * blk_n, blk_n))
                out[part] = (acc[part] * filter_mask[k, i].astype(jnp.float32)).astype(jnp.bfloat16)

    def drain_a(item, carry):
        for way in range(2):
            sign = 1 - 2 * way
            origin = chip - sign * (item // PIECES)
            sent = jnp.logical_and(has_up if way == 0 else has_down, jnp.logical_and(origin >= 0, origin < chips))
            pl.when(sent)(lambda way=way: a_copy(way, item).wait_send())
        return carry

    def drain_b(item, carry):
        for way in range(2):
            b_copy(way, item).wait_send()
        return carry

    def drain_d(index, carry):
        d_copy(index // PIECES, index % PIECES, core).wait_send()
        return carry

    lax.fori_loop(0, a_items, drain_a, 0)
    lax.fori_loop(0, b_items, drain_b, 0)
    lax.fori_loop(0, chips * PIECES, drain_d, 0)


def solution(mesh):
    ring, cols = mesh.shape["row"], mesh.shape["col"]

    def body(density, density_mask, response, response_mask, filter_mask):
        dirs, depth, width = response.shape
        rows, kblock = density.shape
        chips = cols // CORES
        nb = dirs * (depth // kblock) * SPLIT
        a_items = PIECES * (chips - 1)
        b_items = nb * (ring // 2 - 1) + nb // 2
        dma = pltpu.SemaphoreType.DMA
        hbm = pl.BlockSpec(memory_space=pl.ANY)
        masks = (density_mask.T, jnp.swapaxes(response_mask, 1, 2), filter_mask.T)
        return pl.pallas_call(
            functools.partial(kernel, ring, cols),
            out_shape=pltpu.VMEM((dirs, rows, width), jnp.bfloat16),
            in_specs=[hbm] * 5,
            out_specs=pl.BlockSpec(memory_space=pltpu.VMEM),
            scratch_shapes=[
                *(pltpu.SMEM(mask.shape, mask.dtype) for mask in masks),
                pltpu.VMEM((cols, rows, kblock), jnp.bfloat16),
                pltpu.VMEM((ring, dirs, depth, width), jnp.bfloat16),
                pltpu.VMEM((dirs, rows, width), jnp.float32),
                dma((5,)),
                dma((2, a_items)),
                dma((2, a_items)),
                dma((2, b_items)),
                dma((2, b_items)),
                dma((chips, PIECES)),
                dma((chips, PIECES)),
            ],
            compiler_params=pltpu.CompilerParams(collective_id=0, has_side_effects=True),
        )(density, masks[0], response, masks[1], masks[2])

    return jax.shard_map(
        body,
        mesh=mesh,
        in_specs=(P("row", "col"), P("row", "col"), P(None, "row", "col"), P(None, "row", "col"), P("row", "col")),
        out_specs=P(None, "row", "col"),
        check_vma=False,
    )
```

```python
import functools

import jax
import jax.numpy as jnp
from jax import lax
from jax.experimental import pallas as pl
from jax.experimental.pallas import tpu as pltpu
from jax.sharding import PartitionSpec as P

CORES = 2
PIECES = 2
SPLIT = 2
RATIO = PIECES // SPLIT


def kernel(
    ring, cols, density, density_mask_in, response, response_mask_in, filter_mask_in,
    out, density_mask, response_mask, filter_mask, a_full, b_full, acc, load_sem,
    a_send, a_recv, b_send, b_recv, d_send, d_recv,
):
    chips = cols // CORES
    dirs, depth, width = response.shape
    rows, kblock = density.shape
    piece = rows // PIECES
    per = depth // kblock
    thin = depth // SPLIT
    nb = dirs * SPLIT
    far = ring // 2
    a_items = PIECES * (chips - 1)
    b_items = nb * (far - 1) + nb // 2
    blk_r = rows // density_mask.shape[1]
    blk_k = kblock // density_mask.shape[0]

    row = lax.axis_index("row")
    col = lax.axis_index("col")
    chip, core = col // CORES, col % CORES
    partner = chip * CORES + (CORES - 1 - core)

    def row_of(pos):
        pos = lax.rem(pos + 2 * ring, ring)
        return jnp.where(pos < far, 2 * pos, 2 * (ring - 1 - pos) + 1)

    def pos_of(r):
        return jnp.where(r % 2 == 0, r // 2, ring - 1 - r // 2)

    pos = pos_of(row)
    next_row, prev_row = row_of(pos + 1), row_of(pos - 1)
    has_up, has_down = chip < chips - 1, chip > 0

    barrier = pltpu.get_barrier_semaphore()
    pl.semaphore_signal(barrier, inc=1, device_id={"row": next_row})
    pl.semaphore_signal(barrier, inc=1, device_id={"row": prev_row})
    pl.semaphore_signal(barrier, inc=1, device_id={"col": partner})

    @pl.when(has_up)
    def _():
        pl.semaphore_signal(barrier, inc=1, device_id={"col": col + CORES})

    @pl.when(has_down)
    def _():
        pl.semaphore_signal(barrier, inc=1, device_id={"col": col - CORES})

    load_a = pltpu.make_async_copy(density, a_full.at[col], load_sem.at[0])
    load_b = pltpu.make_async_copy(response, b_full.at[row], load_sem.at[1])
    load_masks = [
        pltpu.make_async_copy(source, target, load_sem.at[2 + i])
        for i, (source, target) in enumerate((
            (density_mask_in, density_mask), (response_mask_in, response_mask), (filter_mask_in, filter_mask)))
    ]
    load_a.start()
    load_masks[0].start()
    load_masks[1].start()
    load_b.start()
    load_masks[2].start()
    acc[...] = jnp.zeros_like(acc)
    load_a.wait()
    load_masks[0].wait()
    for i in range(rows // blk_r):
        for k in range(kblock // blk_k):
            part = (col, pl.ds(i * blk_r, blk_r), pl.ds(k * blk_k, blk_k))
            factor = jnp.full((blk_r, blk_k), density_mask[k, i].astype(jnp.float32)).astype(jnp.bfloat16)
            a_full[part] = a_full[part] * factor
    load_b.wait()
    load_masks[1].wait()
    load_masks[2].wait()
    for d in range(dirs):
        for i in range(depth // blk_k):
            for k in range(width // blk_k):
                part = (row, d, pl.ds(i * blk_k, blk_k), pl.ds(k * blk_k, blk_k))
                factor = jnp.full((blk_k, blk_k), response_mask[d, k, i].astype(jnp.float32)).astype(jnp.bfloat16)
                b_full[part] = b_full[part] * factor
    pl.semaphore_wait(barrier, 3 + has_up.astype(jnp.int32) + has_down.astype(jnp.int32))

    def a_copy(way, item):
        step, half = item // PIECES, item % PIECES
        sign = 1 - 2 * way
        origin = (chip - sign * step) * CORES + core
        ref = a_full.at[origin, pl.ds(pl.multiple_of(half * piece, piece), piece)]
        return pltpu.make_async_remote_copy(
            ref, ref, a_send.at[way, item], a_recv.at[way, item],
            device_id={"col": col + sign * CORES},
        )

    def a_arrival(way, item):
        step, half = item // PIECES, item % PIECES
        sign = 1 - 2 * way
        origin = (chip - sign * (step + 1)) * CORES + core
        ref = a_full.at[origin, pl.ds(pl.multiple_of(half * piece, piece), piece)]
        return pltpu.make_async_remote_copy(
            ref, ref, a_send.at[way, item], a_recv.at[way, item],
            device_id={"col": col + sign * CORES},
        )

    def d_copy(origin_chip, half, whose):
        ref = a_full.at[origin_chip * CORES + whose, pl.ds(pl.multiple_of(half * piece, piece), piece)]
        return pltpu.make_async_remote_copy(
            ref, ref, d_send.at[origin_chip, half], d_recv.at[origin_chip, half],
            device_id={"col": partner},
        )

    def b_ref(way, item, origin_pos):
        j = item % nb
        d, s = j // SPLIT, j % SPLIT
        if way == 1:
            d = dirs - 1 - d
        return b_full.at[row_of(origin_pos), d, pl.ds(pl.multiple_of(s * thin, thin), thin)]

    def b_copy(way, item):
        sign = 1 - 2 * way
        ref = b_ref(way, item, pos - sign * (item // nb))
        return pltpu.make_async_remote_copy(
            ref, ref, b_send.at[way, item], b_recv.at[way, item],
            device_id={"row": next_row if way == 0 else prev_row},
        )

    def b_arrival(way, item):
        sign = 1 - 2 * way
        ref = b_ref(way, item, pos - sign * (item // nb + 1))
        return pltpu.make_async_remote_copy(
            ref, ref, b_send.at[way, item], b_recv.at[way, item],
            device_id={"row": next_row if way == 0 else prev_row},
        )

    own_b = min(nb, b_items)
    for item in range(max(own_b, PIECES)):
        if item < PIECES and chips > 1:
            pl.when(has_up)(lambda item=item: a_copy(0, item).start())
            pl.when(has_down)(lambda item=item: a_copy(1, item).start())
        if item < own_b:
            b_copy(0, item).start()
            b_copy(1, item).start()
    for half in range(PIECES):
        d_copy(chip, half, core).start()

    def ready(origin_chip, c, d, source, s):
        late = jnp.where(c == core, 0, 1)
        t_a = PIECES * jnp.abs(origin_chip - chip) + late
        gap = lax.rem(pos - pos_of(source) + ring, ring)
        last = ((s + 1) * kblock - 1) // thin + 1
        from_prev = (gap - 1) * nb + d * SPLIT + last
        from_next = (ring - gap - 1) * nb + (dirs - 1 - d) * SPLIT + last
        up = gap <= far if d < dirs // 2 else gap < far
        t_b = RATIO * jnp.where(gap == 0, 0, jnp.where(up, from_prev, from_next))
        return jnp.maximum(t_a, t_b)

    units = []
    for k in range(cols):
        for d in range(dirs):
            source, s = k // per, k % per
            units.append((k, d, source, s, ready(k // CORES, k % CORES, d, source, s)))

    def compute(tick):
        for k, d, source, s, due in units:

            @pl.when(due == tick)
            def _():
                acc[d] += jnp.dot(
                    a_full[k], b_full[source, d, pl.ds(s * kblock, kblock)], preferred_element_type=jnp.float32
                )

    ticks = max(a_items + 1, RATIO * b_items)

    def arrives(way, item):
        origin = chip - (1 - 2 * way) * (item // PIECES + 1)
        inside = jnp.logical_and(origin >= 0, origin < chips)
        return origin, jnp.logical_and(jnp.logical_and(item >= 0, item < a_items), inside)

    def step(tick, carry):
        item = tick - 1
        for way in range(2):
            origin, here = arrives(way, item)

            @pl.when(here)
            def _():
                a_arrival(way, item).wait_recv()

                @pl.when(has_up if way == 0 else has_down)
                def _():
                    a_copy(way, item + PIECES).start()

                d_copy(origin, item % PIECES, core).start()

        b_item = tick // RATIO - 1

        @pl.when(jnp.logical_and(tick % RATIO == 0, jnp.logical_and(b_item >= 0, b_item < b_items)))
        def _():
            for way in range(2):
                b_arrival(way, b_item).wait_recv()

                @pl.when(b_item + nb < b_items)
                def _():
                    b_copy(way, b_item + nb).start()

        for way in range(2):
            origin, here = arrives(way, item - 1)

            @pl.when(here)
            def _():
                d_copy(origin, (item - 1) % PIECES, CORES - 1 - core).wait_recv()

        @pl.when(tick == 1)
        def _():
            for part in range(PIECES):
                d_copy(chip, part, CORES - 1 - core).wait_recv()

        compute(tick)
        return carry

    lax.fori_loop(0, ticks + 1, step, 0)

    blk_m, blk_n = rows // filter_mask.shape[1], width // filter_mask.shape[0]
    for d in range(dirs):
        for i in range(rows // blk_m):
            for k in range(width // blk_n):
                part = (d, pl.ds(i * blk_m, blk_m), pl.ds(k * blk_n, blk_n))
                out[part] = (acc[part] * filter_mask[k, i].astype(jnp.float32)).astype(jnp.bfloat16)

    def drain_a(item, carry):
        for way in range(2):
            sign = 1 - 2 * way
            origin = chip - sign * (item // PIECES)
            sent = jnp.logical_and(has_up if way == 0 else has_down, jnp.logical_and(origin >= 0, origin < chips))
            pl.when(sent)(lambda way=way: a_copy(way, item).wait_send())
        return carry

    def drain_b(item, carry):
        for way in range(2):
            b_copy(way, item).wait_send()
        return carry

    def drain_d(index, carry):
        d_copy(index // PIECES, index % PIECES, core).wait_send()
        return carry

    lax.fori_loop(0, a_items, drain_a, 0)
    lax.fori_loop(0, b_items, drain_b, 0)
    lax.fori_loop(0, chips * PIECES, drain_d, 0)


def solution(mesh):
    ring, cols = mesh.shape["row"], mesh.shape["col"]

    def body(density, density_mask, response, response_mask, filter_mask):
        dirs, depth, width = response.shape
        rows, kblock = density.shape
        chips = cols // CORES
        nb = dirs * SPLIT
        a_items = PIECES * (chips - 1)
        b_items = nb * (ring // 2 - 1) + nb // 2
        dma = pltpu.SemaphoreType.DMA
        hbm = pl.BlockSpec(memory_space=pl.ANY)
        masks = (density_mask.T, jnp.swapaxes(response_mask, 1, 2), filter_mask.T)
        return pl.pallas_call(
            functools.partial(kernel, ring, cols),
            out_shape=pltpu.VMEM((dirs, rows, width), jnp.bfloat16),
            in_specs=[hbm] * 5,
            out_specs=pl.BlockSpec(memory_space=pltpu.VMEM),
            scratch_shapes=[
                *(pltpu.SMEM(mask.shape, mask.dtype) for mask in masks),
                pltpu.VMEM((cols, rows, kblock), jnp.bfloat16),
                pltpu.VMEM((ring, dirs, depth, width), jnp.bfloat16),
                pltpu.VMEM((dirs, rows, width), jnp.float32),
                dma((5,)),
                dma((2, a_items)),
                dma((2, a_items)),
                dma((2, b_items)),
                dma((2, b_items)),
                dma((chips, PIECES)),
                dma((chips, PIECES)),
            ],
            compiler_params=pltpu.CompilerParams(collective_id=0, has_side_effects=True),
        )(density, masks[0], response, masks[1], masks[2])

    return jax.shard_map(
        body,
        mesh=mesh,
        in_specs=(P("row", "col"), P("row", "col"), P(None, "row", "col"), P(None, "row", "col"), P("row", "col")),
        out_specs=P(None, "row", "col"),
        check_vma=False,
    )
```
